32 devices in a mesh: dp: 4 (over x, core), expert: 8 (over z, y).
Axes of the slice: x: 2, y: 2, z: 4, core: 2. Of those that a mesh axis runs over, the one named last changes fastest.
Arguments:
- tokens: bfloat16 [256, 7168], P('dp', 'expert'), parts along dimension 0, may hold values from -6 to 6
- routes: int32 [256, 8], P('dp'), parts along dimension 0, may hold values from 0 to 15, all different within a row; in each aligned block of 64 rows (0 to 63, 64 to 127, ...) at most 40 rows name the same one
- gate_values: bfloat16 [256, 8], P('dp'), parts along dimension 0, may hold values from 0.049804688 to 1
- gate_weight: bfloat16 [7168, 16384], P(None, 'expert'), may hold values from -0.0625 to 0.0625
- up_weight: bfloat16 [7168, 16384], P(None, 'expert'), may hold values from -0.0625 to 0.0625
- down_weight: bfloat16 [16384, 7168], P(None, 'expert'), may hold values from -0.1875 to 0.1875
Outputs:
- layer_output: bfloat16 [256, 7168], P('dp', 'expert'), parts along dimension 0
The draws below stay inside these ranges and needn't reach their ends.
There are 4 independent parts, one for each index of `dp`. The reference program is written for one: setup_inputs(seed, part) draws one part's arguments, and reference() takes and returns one part's arrays. A program takes and returns all parts, laid end to end along the dimension named above; an argument that names none is the same for every part. Nothing has to cross between parts.
Inputs may be any that keep to these rules, and one draw needn't show every extreme that they name: `routes`: each row names 8 different experts; no expert is named by more than 40 rows of a group, a bound that some block reaches.
All inputs are finite; a program needn't handle non-finite values.
Results may differ from the reference program's by a relative error of at most 0.0049.
Values may be sent and summed in bfloat16 or wider, within the bound.
A program may use at most 128 MiB of HBM per device.

```python
import math
import jax
import jax.numpy as jnp
import numpy as np
from jax import lax

D = 7168
HIDDEN_SIZE = 1024
EXPERTS = 16
TOPK = 8
TOKENS = 64
CAP = 40


def shard_levels(stream_key, dims, pieces, least, largest):
    loudness = 1.0
    for dim, blocks in pieces:
        heights = jax.random.uniform(jax.random.fold_in(jax.random.fold_in(stream_key, 6), dim), (blocks,), jnp.float32, least / len(pieces), largest / len(pieces))
        loudness = loudness * jnp.repeat(jnp.exp(heights), dims[dim] // blocks).reshape((-1,) + (1,) * (len(dims) - 1 - dim))
    return loudness


def deal_out(own_key, own, number, rows, count, top, bound, skew):
    sequence = jax.random.permutation(own_key, count)
    heavy_load, usual = shares(count, rows * top, bound, skew, True), shares(count, rows * top, bound, skew, False)
    places = jnp.arange(count)

    def named(tallies, offset_by):
        used = int((tallies > 0).sum())
        fixed = max(1, used // 4)
        moved = fixed + (places - fixed + offset_by * (used - fixed)) % max(1, count - fixed)
        return jnp.zeros((count,), jnp.int32).at[sequence[jnp.where(places < fixed, places, moved)]].set(jnp.asarray(tallies, jnp.int32))

    tallies = jnp.where(number % 4 == 0, named(heavy_load, number // 4), named(usual, number - number // 4 - 1))
    mixed = jax.random.permutation(jax.random.fold_in(own, 3), count)
    source_of, sink = mixed[0:count // 2 * 2:2], mixed[1:count // 2 * 2:2]
    slack = jnp.minimum(tallies[source_of] - 1, bound - tallies[sink]) // 2
    slack = jnp.where((source_of == sequence[0]) | (sink == sequence[0]) | (tallies[sink] == 0), 0, jnp.maximum(slack, 0))
    moved = jax.random.randint(jax.random.fold_in(own, 4), (count // 2,), 0, 1 << 20) % (slack + 1)
    tallies = tallies.at[source_of].add(-moved).at[sink].add(moved)
    members = jnp.searchsorted(jnp.cumsum(tallies), jnp.arange(rows * top), side="right").astype(jnp.int32)
    table = members.reshape(top, rows).T
    table = table[jax.random.permutation(jax.random.fold_in(own, 1), rows)]
    offset_by = jax.random.randint(jax.random.fold_in(own, 2), (rows, 1), 0, top)
    return jnp.take_along_axis(table, (jnp.arange(top)[None, :] + offset_by) % top, axis=1)


def shares(count, total, most, lean, full):
    portions = [(1 << 20) // math.isqrt(rank ** lean) + 1 for rank in range(1, count + 1)]
    largest = most if full else min(most, max(-(-total // count), total * portions[0] // sum(portions)))
    least = 1 if total - largest >= count - 1 else 0
    given, surplus = [largest] + [least] * (count - 1), total - largest - least * (count - 1)
    while surplus > 0:
        movable = [i for i in range(1, count) if given[i] < largest] or [i for i in range(1, count) if given[i] < most]
        pool, budget = sum([portions[i] for i in movable]), surplus
        for i in movable:
            extra = min(most - given[i], max(1, budget * portions[i] // pool), surplus)
            given[i] = given[i] + extra
            surplus = surplus - extra
    return np.array(given)


def noise(own_key, dims, spread, most, split=(), kind=jnp.bfloat16):
    entries = spread * jax.random.normal(own_key, dims, jnp.float32)
    if split:
        entries = entries * shard_levels(own_key, dims, split, -0.22, 0.18)
    return jnp.clip(entries, -most, most).astype(kind)


def setup_inputs(seed: int = 0, part: int = 0) -> dict:
    splits = jax.random.split(jax.random.key(seed), 7)
    own_keys = jax.random.split(jax.random.fold_in(splits[6], part), 7)
    tokens = noise(own_keys[0], (TOKENS, D), 1.0, 6.0, ((1, 8),))
    routes_keys = jax.random.split(jax.random.fold_in(own_keys[1], 1), TOKENS // TOKENS)
    routes_turns = jax.random.permutation(jax.random.fold_in(own_keys[1], 3), TOKENS // TOKENS)
    routes = jax.vmap(lambda own, number: deal_out(jax.random.fold_in(own_keys[1], 2), own, number, TOKENS, EXPERTS, TOPK, CAP, 1))(routes_keys, routes_turns).reshape((TOKENS, TOPK))
    gate_values = jnp.clip(jnp.exp(jax.random.uniform(own_keys[2], (TOKENS, TOPK), jnp.float32, math.log(0.049804688), math.log(1.0))), 0.049804688, 1.0).astype(jnp.bfloat16)
    gate_weight = noise(splits[3], (D, EXPERTS * HIDDEN_SIZE), D ** -0.5, 0.0625, ((1, 8),))
    up_weight = noise(splits[4], (D, EXPERTS * HIDDEN_SIZE), D ** -0.5, 0.0625, ((1, 8),))
    down_weight = noise(splits[5], (EXPERTS * HIDDEN_SIZE, D), HIDDEN_SIZE ** -0.5, 0.1875, ((1, 8),))
    return {"tokens": tokens, "routes": routes, "gate_values": gate_values, "gate_weight": gate_weight, "up_weight": up_weight, "down_weight": down_weight}


def reference(tokens, routes, gate_values, gate_weight, up_weight, down_weight):
    expert_ids = jnp.arange(EXPERTS, dtype=jnp.int32)
    matched = routes[:, :, None] == expert_ids[None, None, :]
    combine_table = jnp.sum(jnp.where(matched, gate_values[:, :, None].astype(jnp.float32), jnp.float32(0.0)), axis=1)

    def accumulate(totals, expert):
        first_unit = (expert * HIDDEN_SIZE).astype(jnp.int32)
        gate_slab = lax.dynamic_slice_in_dim(gate_weight, first_unit, HIDDEN_SIZE, 1)
        up_slab = lax.dynamic_slice_in_dim(up_weight, first_unit, HIDDEN_SIZE, 1)
        down_slab = lax.dynamic_slice_in_dim(down_weight, first_unit, HIDDEN_SIZE, 0)
        gate_proj = jnp.dot(tokens, gate_slab, preferred_element_type=jnp.float32)
        up_proj = jnp.dot(tokens, up_slab, preferred_element_type=jnp.float32)
        weight = lax.dynamic_slice_in_dim(combine_table, expert, 1, 1)
        hidden = (jax.nn.silu(gate_proj) * up_proj * weight).astype(jnp.bfloat16)
        return totals + jnp.dot(hidden, down_slab, preferred_element_type=jnp.float32), None

    initial = jnp.zeros((tokens.shape[0], tokens.shape[1]), jnp.float32)
    totals, unused = lax.scan(accumulate, initial, expert_ids)
    return totals.astype(jnp.bfloat16)
```

```python
import functools

import jax
import jax.numpy as jnp
from jax import lax
from jax.experimental import pallas as pl
from jax.experimental.pallas import tpu as pltpu
from jax.sharding import PartitionSpec as P

HIDDEN_SIZE = 1024
EXPERTS = 16
CAP = 40
TOKEN_PIECES = 2
HIDDEN_PIECES = 2
MESH = pl.DeviceIdType.MESH


def plain_body(tokens, routes, gate_values, gate_weight, up_weight, down_weight):
    unit_count = gate_weight.shape[1]
    span_units = min(unit_count, HIDDEN_SIZE)
    local_count = unit_count // span_units
    token_count = tokens.shape[0]
    first_expert = lax.axis_index("expert") * unit_count // HIDDEN_SIZE
    matched = routes[:, :, None] == lax.broadcasted_iota(jnp.int32, (1, 1, EXPERTS), 2)
    combine_table = jnp.sum(
        jnp.where(matched, gate_values[:, :, None].astype(jnp.float32), 0.0), axis=1
    )
    selector = (
        lax.broadcasted_iota(jnp.int32, (EXPERTS, local_count), 0)
        == first_expert + lax.broadcasted_iota(jnp.int32, (EXPERTS, local_count), 1)
    ).astype(jnp.float32)
    local_gates = jnp.dot(
        combine_table, selector, precision=lax.Precision.HIGHEST, preferred_element_type=jnp.float32
    )
    all_rows = lax.all_gather(tokens, "expert", axis=1, tiled=True)
    gate_proj = jnp.dot(all_rows, gate_weight, preferred_element_type=jnp.float32)
    up_proj = jnp.dot(all_rows, up_weight, preferred_element_type=jnp.float32)
    product = (jax.nn.silu(gate_proj) * up_proj).reshape(token_count, local_count, span_units)
    product = product * local_gates[:, :, None]
    hidden = product.reshape(token_count, unit_count).astype(jnp.bfloat16)
    result = jnp.dot(
        lax.all_gather(hidden, "expert", axis=1, tiled=True),
        down_weight,
        preferred_element_type=jnp.float32,
    )
    return result.astype(jnp.bfloat16)


def xor(a, b, bits):
    total = 0
    for i in range(bits):
        p, q = (a // 2**i) % 2, (b // 2**i) % 2
        total = total + (p + q - 2 * p * q) * 2**i
    return total


def kernel(
    n,
    tokens_hbm, routes_hbm, values_hbm, gate_hbm, up_hbm, down_hbm, out_ref,
    x_buf, r_buf, v_buf, wg, wu, wd, h_buf, acc_g, acc_u, acc_o, other_o, slots,
    local_sem, wg_sem, wu_sem, wd_sem,
    xz_send, xy_send, xd_send, x_recv, xd_recv,
    rv_send, rv_recv, hz_send, hy_send, h_recv, o_send, o_recv,
):
    d, e = lax.axis_index("dp"), lax.axis_index("expert")
    core = d % 2
    row, side = e // 2, e % 2
    lines = n // 2
    bits = lines.bit_length() - 1
    rows, cols = x_buf.shape[2], x_buf.shape[3]
    units = wg.shape[2]
    both = 2 * rows
    cap = h_buf.shape[2]
    mate = {"dp": d + 1 - 2 * core}
    f32, bf16 = jnp.float32, jnp.bfloat16

    def source(k, crossed):
        return 2 * xor(row, k, bits) + xor(side, crossed, 1)

    def target(k, crossed):
        return {"expert": source(k, crossed)}

    def weight_copies(i):
        who = source(i // 2, i % 2)
        at = pl.ds(pl.multiple_of(who * cols, cols), cols)
        mine = pl.ds(pl.multiple_of(core * units, units), units)
        return (
            pltpu.make_async_copy(gate_hbm.at[at, mine], wg.at[who], wg_sem.at[who]),
            pltpu.make_async_copy(up_hbm.at[at, mine], wu.at[who], wu_sem.at[who]),
        )

    def down_copy(i):
        who = source(i // 2, i % 2)
        at = pl.ds(pl.multiple_of((2 * who + core) * units, units), units)
        return pltpu.make_async_copy(down_hbm.at[at, :], wd.at[who], wd_sem.at[who])

    own_copies = (
        pltpu.make_async_copy(tokens_hbm, x_buf.at[core, e], local_sem.at[0]),
        pltpu.make_async_copy(routes_hbm, r_buf.at[core], local_sem.at[1]),
        pltpu.make_async_copy(values_hbm, v_buf.at[core], local_sem.at[2]),
    )
    for copy in own_copies:
        copy.start()
    for i in range(n):
        for copy in weight_copies(i):
            copy.start()
    for i in range(n):
        down_copy(i).start()

    barrier = pltpu.get_barrier_semaphore()
    for k in range(1, lines):
        pl.semaphore_signal(barrier, inc=1, device_id=target(k, 0), device_id_type=MESH)
    pl.semaphore_signal(barrier, inc=1, device_id=target(0, 1), device_id_type=MESH)
    pl.semaphore_signal(barrier, inc=1, device_id=mate, device_id_type=MESH)
    pl.semaphore_wait(barrier, lines + 1)

    def remote(src, send, recv, device):
        return pltpu.make_async_remote_copy(
            src_ref=src, dst_ref=src, send_sem=send, recv_sem=recv,
            device_id=device, device_id_type=MESH,
        )

    part = rows // TOKEN_PIECES

    def x_piece(who, p):
        return x_buf.at[core, who, pl.ds(p * part, part)]

    def x_along(k, p):
        return remote(x_piece(e, p), xz_send.at[k, p], x_recv.at[e, p], target(k, 0))

    def x_across(k, p):
        who = source(k, 0)
        return remote(x_piece(who, p), xy_send.at[k, p], x_recv.at[who, p], target(0, 1))

    def x_share(who, p):
        return remote(x_piece(who, p), xd_send.at[who, p], xd_recv.at[who, p], mate)

    def x_arrival(who, p):
        return remote(x_piece(who, p), xd_send.at[who, p], x_recv.at[who, p], mate)

    def x_shared(who, p):
        there = x_buf.at[1 - core, who, pl.ds(p * part, part)]
        return remote(there, xd_send.at[who, p], xd_recv.at[who, p], mate)

    r_share = remote(r_buf.at[core], rv_send.at[0], rv_recv.at[0], mate)
    v_share = remote(v_buf.at[core], rv_send.at[1], rv_recv.at[1], mate)

    for copy in own_copies:
        copy.wait()
    for p in range(TOKEN_PIECES):
        x_across(0, p).start()
        for k in range(1, lines):
            x_along(k, p).start()
        x_share(e, p).start()
    r_share.start()
    v_share.start()
    acc_g[...] = jnp.zeros_like(acc_g)
    acc_u[...] = jnp.zeros_like(acc_u)
    acc_o[...] = jnp.zeros_like(acc_o)
    r_share.wait_recv()
    v_share.wait_recv()

    lane = lax.broadcasted_iota(jnp.int32, (both, 128), 1)
    routed = r_buf[...].reshape(both, r_buf.shape[2])
    values = v_buf[...].astype(f32).reshape(both, v_buf.shape[2])
    named = jnp.zeros((both, 128), f32)
    combine = jnp.zeros((both, 128), f32)
    for k in range(routed.shape[1]):
        hit = routed[:, k:k + 1] == lane
        named = jnp.where(hit, 1.0, named)
        combine = combine + jnp.where(hit, values[:, k:k + 1], 0.0)
    t0 = lax.broadcasted_iota(jnp.int32, (both, both), 0)
    t1 = lax.broadcasted_iota(jnp.int32, (both, both), 1)
    earlier = jnp.where((t1 < t0) & ((t1 >= rows) == (t0 >= rows)), 1.0, 0.0)
    rank = jnp.dot(earlier.astype(bf16), named.astype(bf16), preferred_element_type=f32)
    base = jnp.where(lax.broadcasted_iota(jnp.int32, (both, 128), 0) >= rows, float(CAP), 0.0)
    table = jnp.where(named > 0.0, rank + base, -1.0)
    slots[...] = table
    expert = 2 * e + core
    sub = lax.broadcasted_iota(jnp.int32, (128, both), 0)
    slot_row = jnp.sum(jnp.where(sub == expert, table.T, 0.0), axis=0, keepdims=True)
    value_row = jnp.sum(jnp.where(sub == expert, combine.T, 0.0), axis=0, keepdims=True)
    picked = slot_row == lax.broadcasted_iota(jnp.int32, (cap, both), 0).astype(f32)
    pick = jnp.where(picked, 1.0, 0.0).astype(bf16)
    weight = jnp.sum(jnp.where(picked, value_row, 0.0), axis=1, keepdims=True)

    def gate_step(j, carry):
        k, crossed = j // 2, j % 2
        who = source(k, crossed)

        @pl.when((crossed == 1) & (k + 1 < lines))
        def _():
            for p in range(TOKEN_PIECES):
                coming = source(k + 1, 0)
                x_arrival(coming, p).wait_recv()
                x_across(k + 1, p).start()
                x_share(coming, p).start()

        @pl.when(crossed == 1)
        def _():
            for p in range(TOKEN_PIECES):
                x_arrival(who, p).wait_recv()
                x_share(who, p).start()

        for p in range(TOKEN_PIECES):
            x_shared(who, p).wait_recv()
        for copy in weight_copies(j):
            copy.wait()
        x = jnp.concatenate([x_buf[0, who], x_buf[1, who]], axis=0)
        xc = jnp.dot(pick, x, preferred_element_type=f32).astype(bf16)
        acc_g[...] += jnp.dot(xc, wg[who], preferred_element_type=f32)
        acc_u[...] += jnp.dot(xc, wu[who], preferred_element_type=f32)
        return carry

    lax.fori_loop(0, n, gate_step, 0)

    def h_along(k, p):
        return remote(h_buf.at[e, p], hz_send.at[k, p], h_recv.at[e, p], target(k, 0))

    def h_across(k, p):
        who = source(k, 0)
        return remote(h_buf.at[who, p], hy_send.at[k, p], h_recv.at[who, p], target(0, 1))

    def h_arrival(who, p):
        return remote(h_buf.at[who, p], hy_send.at[0, p], h_recv.at[who, p], target(0, 1))

    slab = units // HIDDEN_PIECES
    for p in range(HIDDEN_PIECES):
        at = slice(p * slab, (p + 1) * slab)
        gate = acc_g[:, at]
        hidden = gate / (1.0 + jnp.exp(-gate)) * acc_u[:, at] * weight
        h_buf[e, p] = hidden.astype(bf16)
        h_across(0, p).start()
        for k in range(1, lines):
            h_along(k, p).start()

    def down_step(j, carry):
        k, crossed = j // 2, j % 2
        who = source(k, crossed)

        @pl.when((crossed == 1) & (k + 1 < lines))
        def _():
            for p in range(HIDDEN_PIECES):
                h_arrival(source(k + 1, 0), p).wait_recv()
                h_across(k + 1, p).start()

        @pl.when(crossed == 1)
        def _():
            for p in range(HIDDEN_PIECES):
                h_arrival(who, p).wait_recv()

        down_copy(j).wait()
        lanes = lax.broadcasted_iota(jnp.int32, (both, 128), 1)
        column = jnp.sum(
            jnp.where(lanes == 2 * who + core, slots[...], 0.0), axis=1, keepdims=True
        )
        place = column == lax.broadcasted_iota(jnp.int32, (both, cap), 1).astype(f32)
        place = jnp.where(place, 1.0, 0.0).astype(bf16)
        for p in range(HIDDEN_PIECES):
            full = jnp.dot(place, h_buf[who, p], preferred_element_type=f32).astype(bf16)
            acc_o[...] += jnp.dot(
                full, wd[who, pl.ds(p * slab, slab)], preferred_element_type=f32
            ).reshape(acc_o.shape)
        return carry

    lax.fori_loop(0, n, down_step, 0)

    back = pltpu.make_async_remote_copy(
        src_ref=acc_o.at[1 - core], dst_ref=other_o, send_sem=o_send, recv_sem=o_recv,
        device_id=mate, device_id_type=MESH,
    )
    back.start()
    r_share.wait_send()
    v_share.wait_send()
    for p in range(TOKEN_PIECES):
        for k in range(lines):
            x_across(k, p).wait_send()
        for k in range(1, lines):
            x_along(k, p).wait_send()
        for i in range(n):
            x_share(i, p).wait_send()
    for p in range(HIDDEN_PIECES):
        for k in range(lines):
            h_across(k, p).wait_send()
        for k in range(1, lines):
            h_along(k, p).wait_send()
    back.wait()
    out_ref[...] = (acc_o[core] + other_o[...]).astype(out_ref.dtype)


def fused_body(n, tokens, routes, gate_values, gate_weight, up_weight, down_weight):
    rows, cols = tokens.shape
    units = gate_weight.shape[1] // 2
    cap = 2 * CAP
    lines = n // 2
    dma = lambda *dims: pltpu.SemaphoreType.DMA(dims)
    bf16, f32 = jnp.bfloat16, jnp.float32
    return pl.pallas_call(
        functools.partial(kernel, n),
        out_shape=jax.ShapeDtypeStruct((rows, cols), bf16),
        in_specs=[pl.BlockSpec(memory_space=pl.ANY)] * 6,
        out_specs=pl.BlockSpec(memory_space=pltpu.VMEM),
        scratch_shapes=[
            pltpu.VMEM((2, n, rows, cols), bf16),
            pltpu.VMEM((2,) + routes.shape, routes.dtype),
            pltpu.VMEM((2,) + gate_values.shape, bf16),
            pltpu.VMEM((n, cols, units), bf16),
            pltpu.VMEM((n, cols, units), bf16),
            pltpu.VMEM((n, units, cols), bf16),
            pltpu.VMEM((n, HIDDEN_PIECES, cap, units // HIDDEN_PIECES), bf16),
            pltpu.VMEM((cap, units), f32),
            pltpu.VMEM((cap, units), f32),
            pltpu.VMEM((2, rows, cols), f32),
            pltpu.VMEM((rows, cols), f32),
            pltpu.VMEM((2 * rows, 128), f32),
            dma(3), dma(n), dma(n), dma(n),
            dma(lines, TOKEN_PIECES), dma(lines, TOKEN_PIECES), dma(n, TOKEN_PIECES),
            dma(n, TOKEN_PIECES), dma(n, TOKEN_PIECES),
            dma(2), dma(2),
            dma(lines, HIDDEN_PIECES), dma(lines, HIDDEN_PIECES), dma(n, HIDDEN_PIECES),
            pltpu.SemaphoreType.DMA, pltpu.SemaphoreType.DMA,
        ],
        compiler_params=pltpu.CompilerParams(
            collective_id=0, has_side_effects=True, vmem_limit_bytes=62 * 1024 * 1024
        ),
    )(tokens, routes, gate_values, gate_weight, up_weight, down_weight)


def solution(mesh):
    in_specs = (
        P("dp", "expert"),
        P("dp", None),
        P("dp", None),
        P(None, "expert"),
        P(None, "expert"),
        P(None, "expert"),
    )
    out_specs = P("dp", "expert")
    n = mesh.shape["expert"]
    lines = n // 2

    def body(*args):
        tokens, gate_weight = args[0], args[3]
        whole_experts = gate_weight.shape[1] == 2 * HIDDEN_SIZE
        aligned = tokens.shape[1] % 128 == 0 and 2 * tokens.shape[0] == 128
        paired = mesh.shape["dp"] % 2 == 0 and n % 2 == 0 and lines & (lines - 1) == 0
        if whole_experts and aligned and paired and lines > 1:
            return fused_body(n, *args)
        return plain_body(*args)

    return jax.shard_map(body, mesh=mesh, in_specs=in_specs, out_specs=out_specs, check_vma=False)
```

```python
import functools

import jax
import jax.numpy as jnp
from jax import lax
from jax.experimental import pallas as pl
from jax.experimental.pallas import tpu as pltpu
from jax.sharding import PartitionSpec as P

HIDDEN_SIZE = 1024
EXPERTS = 16
CAP = 40
TOKEN_PIECES = 1
HIDDEN_PIECES = 1
MESH = pl.DeviceIdType.MESH


def plain_body(tokens, routes, gate_values, gate_weight, up_weight, down_weight):
    unit_count = gate_weight.shape[1]
    span_units = min(unit_count, HIDDEN_SIZE)
    local_count = unit_count // span_units
    token_count = tokens.shape[0]
    first_expert = lax.axis_index("expert") * unit_count // HIDDEN_SIZE
    matched = routes[:, :, None] == lax.broadcasted_iota(jnp.int32, (1, 1, EXPERTS), 2)
    combine_table = jnp.sum(
        jnp.where(matched, gate_values[:, :, None].astype(jnp.float32), 0.0), axis=1
    )
    selector = (
        lax.broadcasted_iota(jnp.int32, (EXPERTS, local_count), 0)
        == first_expert + lax.broadcasted_iota(jnp.int32, (EXPERTS, local_count), 1)
    ).astype(jnp.float32)
    local_gates = jnp.dot(
        combine_table, selector, precision=lax.Precision.HIGHEST, preferred_element_type=jnp.float32
    )
    all_rows = lax.all_gather(tokens, "expert", axis=1, tiled=True)
    gate_proj = jnp.dot(all_rows, gate_weight, preferred_element_type=jnp.float32)
    up_proj = jnp.dot(all_rows, up_weight, preferred_element_type=jnp.float32)
    product = (jax.nn.silu(gate_proj) * up_proj).reshape(token_count, local_count, span_units)
    product = product * local_gates[:, :, None]
    hidden = product.reshape(token_count, unit_count).astype(jnp.bfloat16)
    result = jnp.dot(
        lax.all_gather(hidden, "expert", axis=1, tiled=True),
        down_weight,
        preferred_element_type=jnp.float32,
    )
    return result.astype(jnp.bfloat16)


def xor(a, b, bits):
    total = 0
    for i in range(bits):
        p, q = (a // 2**i) % 2, (b // 2**i) % 2
        total = total + (p + q - 2 * p * q) * 2**i
    return total


def kernel(
    n,
    tokens_hbm, routes_hbm, values_hbm, gate_hbm, up_hbm, down_hbm, out_ref,
    x_buf, r_buf, v_buf, wg, wu, wd, h_buf, acc_g, acc_u, acc_o, other_o, slots,
    local_sem, wg_sem, wu_sem, wd_sem,
    xz_send, xy_send, xd_send, x_recv, xd_recv,
    rv_send, rv_recv, hz_send, hy_send, h_recv, o_send, o_recv,
):
    d, e = lax.axis_index("dp"), lax.axis_index("expert")
    core = d % 2
    row, side = e // 2, e % 2
    lines = n // 2
    bits = lines.bit_length() - 1
    rows, cols = x_buf.shape[2], x_buf.shape[3]
    units = wg.shape[2]
    both = 2 * rows
    cap = h_buf.shape[2]
    mate = {"dp": d + 1 - 2 * core}
    f32, bf16 = jnp.float32, jnp.bfloat16

    def source(k, crossed):
        return 2 * xor(row, k, bits) + xor(side, crossed, 1)

    def target(k, crossed):
        return {"expert": source(k, crossed)}

    def weight_copies(i):
        who = source(i // 2, i % 2)
        at = pl.ds(pl.multiple_of(who * cols, cols), cols)
        mine = pl.ds(pl.multiple_of(core * units, units), units)
        return (
            pltpu.make_async_copy(gate_hbm.at[at, mine], wg.at[who], wg_sem.at[who]),
            pltpu.make_async_copy(up_hbm.at[at, mine], wu.at[who], wu_sem.at[who]),
        )

    def down_copy(i):
        who = source(i // 2, i % 2)
        at = pl.ds(pl.multiple_of((2 * who + core) * units, units), units)
        return pltpu.make_async_copy(down_hbm.at[at, :], wd.at[who], wd_sem.at[who])

    own_copies = (
        pltpu.make_async_copy(tokens_hbm, x_buf.at[core, e], local_sem.at[0]),
        pltpu.make_async_copy(routes_hbm, r_buf.at[core], local_sem.at[1]),
        pltpu.make_async_copy(values_hbm, v_buf.at[core], local_sem.at[2]),
    )
    for copy in own_copies:
        copy.start()

    barrier = pltpu.get_barrier_semaphore()
    for k in range(1, lines):
        pl.semaphore_signal(barrier, inc=1, device_id=target(k, 0), device_id_type=MESH)
    pl.semaphore_signal(barrier, inc=1, device_id=target(0, 1), device_id_type=MESH)
    pl.semaphore_signal(barrier, inc=1, device_id=mate, device_id_type=MESH)
    pl.semaphore_wait(barrier, lines + 1)

    def remote(src, send, recv, device):
        return pltpu.make_async_remote_copy(
            src_ref=src, dst_ref=src, send_sem=send, recv_sem=recv,
            device_id=device, device_id_type=MESH,
        )

    part = rows // TOKEN_PIECES

    def x_piece(who, p):
        return x_buf.at[core, who, pl.ds(p * part, part)]

    def x_along(k, p):
        return remote(x_piece(e, p), xz_send.at[k, p], x_recv.at[e, p], target(k, 0))

    def x_across(k, p):
        who = source(k, 0)
        return remote(x_piece(who, p), xy_send.at[k, p], x_recv.at[who, p], target(0, 1))

    def x_share(who, p):
        return remote(x_piece(who, p), xd_send.at[who, p], xd_recv.at[who, p], mate)

    def x_arrival(who, p):
        return remote(x_piece(who, p), xd_send.at[who, p], x_recv.at[who, p], mate)

    def x_shared(who, p):
        there = x_buf.at[1 - core, who, pl.ds(p * part, part)]
        return remote(there, xd_send.at[who, p], xd_recv.at[who, p], mate)

    r_share = remote(r_buf.at[core], rv_send.at[0], rv_recv.at[0], mate)
    v_share = remote(v_buf.at[core], rv_send.at[1], rv_recv.at[1], mate)

    for copy in own_copies:
        copy.wait()
    for p in range(TOKEN_PIECES):
        x_across(0, p).start()
        for k in range(1, lines):
            x_along(k, p).start()
        x_share(e, p).start()
    r_share.start()
    v_share.start()
    for i in range(n):
        for copy in weight_copies(i):
            copy.start()
    acc_g[...] = jnp.zeros_like(acc_g)
    acc_u[...] = jnp.zeros_like(acc_u)
    acc_o[...] = jnp.zeros_like(acc_o)
    r_share.wait_recv()
    v_share.wait_recv()

    named = []
    combine = []
    for g in range(2):
        expert_row = lax.broadcasted_iota(jnp.int32, (128, rows), 0)
        hits = jnp.zeros((128, rows), f32)
        shares = jnp.zeros((128, rows), f32)
        values = v_buf[g].astype(f32)
        for k in range(r_buf.shape[1]):
            hit = r_buf[g, k:k + 1, :] == expert_row
            hits = jnp.where(hit, 1.0, hits)
            shares = jnp.where(hit, values[k:k + 1, :], shares)
        named.append(hits)
        combine.append(shares)
    named = jnp.concatenate(named, axis=1)
    combine = jnp.concatenate(combine, axis=1)
    t0 = lax.broadcasted_iota(jnp.int32, (both, both), 0)
    t1 = lax.broadcasted_iota(jnp.int32, (both, both), 1)
    earlier = jnp.where((t0 < t1) & ((t0 >= rows) == (t1 >= rows)), 1.0, 0.0)
    rank = jnp.dot(named.astype(bf16), earlier.astype(bf16), preferred_element_type=f32)
    base = jnp.where(lax.broadcasted_iota(jnp.int32, (128, both), 1) >= rows, float(CAP), 0.0)
    table = jnp.where(named > 0.0, rank + base, -1.0)
    slots[...] = table.T
    expert = 2 * e + core
    sub = lax.broadcasted_iota(jnp.int32, (128, both), 0)
    slot_row = jnp.sum(jnp.where(sub == expert, table, 0.0), axis=0, keepdims=True)
    value_row = jnp.sum(jnp.where(sub == expert, combine, 0.0), axis=0, keepdims=True)
    picked = slot_row == lax.broadcasted_iota(jnp.int32, (cap, both), 0).astype(f32)
    pick = jnp.where(picked, 1.0, 0.0).astype(bf16)
    weight = jnp.sum(jnp.where(picked, value_row, 0.0), axis=1, keepdims=True)

    def gate_step(j, carry):
        k, crossed = j // 2, j % 2
        who = source(k, crossed)

        @pl.when((crossed == 1) & (k + 1 < lines))
        def _():
            for p in range(TOKEN_PIECES):
                coming = source(k + 1, 0)
                x_arrival(coming, p).wait_recv()
                x_across(k + 1, p).start()
                x_share(coming, p).start()

        @pl.when(crossed == 1)
        def _():
            for p in range(TOKEN_PIECES):
                x_arrival(who, p).wait_recv()
                x_share(who, p).start()

        for p in range(TOKEN_PIECES):
            x_shared(who, p).wait_recv()
        for copy in weight_copies(j):
            copy.wait()
        down_copy(j).start()
        x = jnp.concatenate([x_buf[0, who], x_buf[1, who]], axis=0)
        xc = jnp.dot(pick, x, preferred_element_type=f32).astype(bf16)
        acc_g[...] += jnp.dot(xc, wg[who], preferred_element_type=f32)
        acc_u[...] += jnp.dot(xc, wu[who], preferred_element_type=f32)
        return carry

    lax.fori_loop(0, n, gate_step, 0)

    def h_along(k, p):
        return remote(h_buf.at[e, p], hz_send.at[k, p], h_recv.at[e, p], target(k, 0))

    def h_across(k, p):
        who = source(k, 0)
        return remote(h_buf.at[who, p], hy_send.at[k, p], h_recv.at[who, p], target(0, 1))

    def h_arrival(who, p):
        return remote(h_buf.at[who, p], hy_send.at[0, p], h_recv.at[who, p], target(0, 1))

    slab = units // HIDDEN_PIECES
    for p in range(HIDDEN_PIECES):
        at = slice(p * slab, (p + 1) * slab)
        gate = acc_g[:, at]
        hidden = gate / (1.0 + jnp.exp(-gate)) * acc_u[:, at] * weight
        h_buf[e, p] = hidden.astype(bf16)
        h_across(0, p).start()
        for k in range(1, lines):
            h_along(k, p).start()

    def down_step(j, carry):
        k, crossed = j // 2, j % 2
        who = source(k, crossed)

        @pl.when((crossed == 1) & (k + 1 < lines))
        def _():
            for p in range(HIDDEN_PIECES):
                h_arrival(source(k + 1, 0), p).wait_recv()
                h_across(k + 1, p).start()

        @pl.when(crossed == 1)
        def _():
            for p in range(HIDDEN_PIECES):
                h_arrival(who, p).wait_recv()

        down_copy(j).wait()
        lanes = lax.broadcasted_iota(jnp.int32, (both, 128), 1)
        column = jnp.sum(
            jnp.where(lanes == 2 * who + core, slots[...], 0.0), axis=1, keepdims=True
        )
        place = column == lax.broadcasted_iota(jnp.int32, (both, cap), 1).astype(f32)
        place = jnp.where(place, 1.0, 0.0).astype(bf16)
        for p in range(HIDDEN_PIECES):
            full = jnp.dot(place, h_buf[who, p], preferred_element_type=f32).astype(bf16)
            acc_o[...] += jnp.dot(
                full, wd[who, pl.ds(p * slab, slab)], preferred_element_type=f32
            ).reshape(acc_o.shape)
        return carry

    lax.fori_loop(0, n, down_step, 0)

    back = pltpu.make_async_remote_copy(
        src_ref=acc_o.at[1 - core], dst_ref=other_o, send_sem=o_send, recv_sem=o_recv,
        device_id=mate, device_id_type=MESH,
    )
    back.start()
    r_share.wait_send()
    v_share.wait_send()
    for p in range(TOKEN_PIECES):
        for k in range(lines):
            x_across(k, p).wait_send()
        for k in range(1, lines):
            x_along(k, p).wait_send()
        for i in range(n):
            x_share(i, p).wait_send()
    for p in range(HIDDEN_PIECES):
        for k in range(lines):
            h_across(k, p).wait_send()
        for k in range(1, lines):
            h_along(k, p).wait_send()
    back.wait()
    out_ref[...] = (acc_o[core] + other_o[...]).astype(out_ref.dtype)


def fused_body(n, tokens, routes, gate_values, gate_weight, up_weight, down_weight):
    rows, cols = tokens.shape
    units = gate_weight.shape[1] // 2
    cap = 2 * CAP
    lines = n // 2
    dma = lambda *dims: pltpu.SemaphoreType.DMA(dims)
    bf16, f32 = jnp.bfloat16, jnp.float32
    return pl.pallas_call(
        functools.partial(kernel, n),
        out_shape=jax.ShapeDtypeStruct((rows, cols), bf16),
        in_specs=[pl.BlockSpec(memory_space=pl.ANY)] * 6,
        out_specs=pl.BlockSpec(memory_space=pltpu.VMEM),
        scratch_shapes=[
            pltpu.VMEM((2, n, rows, cols), bf16),
            pltpu.VMEM((2,) + routes.shape[::-1], routes.dtype),
            pltpu.VMEM((2,) + gate_values.shape[::-1], bf16),
            pltpu.VMEM((n, cols, units), bf16),
            pltpu.VMEM((n, cols, units), bf16),
            pltpu.VMEM((n, units, cols), bf16),
            pltpu.VMEM((n, HIDDEN_PIECES, cap, units // HIDDEN_PIECES), bf16),
            pltpu.VMEM((cap, units), f32),
            pltpu.VMEM((cap, units), f32),
            pltpu.VMEM((2, rows, cols), f32),
            pltpu.VMEM((rows, cols), f32),
            pltpu.VMEM((2 * rows, 128), f32),
            dma(3), dma(n), dma(n), dma(n),
            dma(lines, TOKEN_PIECES), dma(lines, TOKEN_PIECES), dma(n, TOKEN_PIECES),
            dma(n, TOKEN_PIECES), dma(n, TOKEN_PIECES),
            dma(2), dma(2),
            dma(lines, HIDDEN_PIECES), dma(lines, HIDDEN_PIECES), dma(n, HIDDEN_PIECES),
            pltpu.SemaphoreType.DMA, pltpu.SemaphoreType.DMA,
        ],
        compiler_params=pltpu.CompilerParams(
            collective_id=0, has_side_effects=True, vmem_limit_bytes=62 * 1024 * 1024
        ),
    )(tokens, routes.T, gate_values.T, gate_weight, up_weight, down_weight)


def solution(mesh):
    in_specs = (
        P("dp", "expert"),
        P("dp", None),
        P("dp", None),
        P(None, "expert"),
        P(None, "expert"),
        P(None, "expert"),
    )
    out_specs = P("dp", "expert")
    n = mesh.shape["expert"]
    lines = n // 2

    def body(*args):
        tokens, gate_weight = args[0], args[3]
        whole_experts = gate_weight.shape[1] == 2 * HIDDEN_SIZE
        aligned = tokens.shape[1] % 128 == 0 and 2 * tokens.shape[0] == 128
        paired = mesh.shape["dp"] % 2 == 0 and n % 2 == 0 and lines & (lines - 1) == 0
        if whole_experts and aligned and paired and lines > 1:
            return fused_body(n, *args)
        return plain_body(*args)

    return jax.shard_map(body, mesh=mesh, in_specs=in_specs, out_specs=out_specs, check_vma=False)
```
